16 devices in a mesh: tp: 2 (over z), dp: 8 (over y, x, core).
Axes of the slice: x: 2, y: 2, z: 2, core: 2. Of those that a mesh axis runs over, the one named last changes fastest.
Arguments:
- hid_q: bfloat16 [128, 512, 1024], P('dp')
- hid_d: bfloat16 [512, 512, 1024], P('dp')
- len_q: int32 [128], P('dp')
- len_d: int32 [512], P('dp')
- pos_doc: int32 [128], P('dp')
- w_q: bfloat16 [1024, 2048], P(None, 'tp')
- w_k: bfloat16 [1024, 1024], P(None, 'tp')
- w_v: bfloat16 [1024, 1024], P(None, 'tp')
- w_o: bfloat16 [2048, 1024], P('tp')
- w_gate: bfloat16 [1024, 3072], P(None, 'tp')
- w_up: bfloat16 [1024, 3072], P(None, 'tp')
- w_down: bfloat16 [3072, 1024], P('tp')
- g_in: bfloat16 [1024], replicated
- g_q: bfloat16 [128], replicated
- g_k: bfloat16 [128], replicated
- g_post: bfloat16 [1024], replicated
- g_final: bfloat16 [1024], replicated
Outputs:
- output 1: float32 [128], P('dp')
- output 2: bfloat16 [128, 512, 1024], P('dp')
- output 3: bfloat16 [512, 512, 1024], P('dp')
- output 4: float32 [1024, 2048], P(None, 'tp')
- output 5: float32 [1024, 1024], P(None, 'tp')
- output 6: float32 [1024, 1024], P(None, 'tp')
- output 7: float32 [2048, 1024], P('tp')
- output 8: float32 [1024, 3072], P(None, 'tp')
- output 9: float32 [1024, 3072], P(None, 'tp')
- output 10: float32 [3072, 1024], P('tp')
- output 11: float32 [1024], replicated
- output 12: float32 [128], replicated
- output 13: float32 [128], replicated
- output 14: float32 [1024], replicated
- output 15: float32 [1024], replicated
All inputs are finite; a program needn't handle non-finite values.
Results may differ from the reference program's by a relative error of at most 0.02.
Values sent between devices are 32-bit elements.
A program may use at most 1 GiB of HBM per device.

```python
import jax
import jax.numpy as jnp
from jax import lax

N_QRY = 128
N_DOC = 512
SEQ_LEN = 512
D_MODEL = 1024
HEADS = 16
KV_HEADS = 8
HEAD_DIM = 128
FF_DIM = 3072

NORM_EPS = 1e-6
ROPE_THETA = 1000000.0
TEMPERATURE = 0.05
POS_MIX = 0.3


def dense_init(rng_key, fan_in, fan_out):
    return (jax.random.normal(rng_key, (fan_in, fan_out), jnp.float32) * fan_in ** -0.5).astype(jnp.bfloat16)


def gain_init(rng_key, n_width):
    return (1.0 + 0.3 * jax.random.normal(rng_key, (n_width,), jnp.float32)).astype(jnp.bfloat16)


def setup_inputs(seed: int = 0) -> dict:
    rng_keys = jax.random.split(jax.random.key(seed), 17)
    q_max = SEQ_LEN // 4
    len_q = jax.random.randint(rng_keys[0], (N_QRY,), 1, q_max + 1).at[0].set(q_max).at[1].set(1)
    len_d = jax.random.randint(rng_keys[1], (N_DOC,), 1, SEQ_LEN + 1).at[0].set(SEQ_LEN).at[1].set(1)
    pos_doc = jax.random.randint(rng_keys[2], (N_QRY,), 0, N_DOC).at[0].set(N_DOC - 1).at[1].set(0)
    hid_d = jax.random.normal(rng_keys[3], (N_DOC, SEQ_LEN, D_MODEL), jnp.float32)
    hid_q = jax.random.normal(rng_keys[4], (N_QRY, SEQ_LEN, D_MODEL), jnp.float32)
    target = hid_d[pos_doc, len_d[pos_doc] - 1]
    at_last = (jnp.arange(SEQ_LEN)[None, :] == (len_q - 1)[:, None])[:, :, None]
    mixed_q = (1.0 - POS_MIX ** 2) ** 0.5 * hid_q + POS_MIX * target[:, None, :]
    hid_q = jnp.where(at_last, mixed_q, hid_q)
    q_width = HEADS * HEAD_DIM
    kv_width = KV_HEADS * HEAD_DIM
    return {
        'hid_q': hid_q.astype(jnp.bfloat16),
        'hid_d': hid_d.astype(jnp.bfloat16),
        'len_q': len_q,
        'len_d': len_d,
        'pos_doc': pos_doc,
        'w_q': dense_init(rng_keys[5], D_MODEL, q_width),
        'w_k': dense_init(rng_keys[6], D_MODEL, kv_width),
        'w_v': dense_init(rng_keys[7], D_MODEL, kv_width),
        'w_o': dense_init(rng_keys[8], q_width, D_MODEL),
        'w_gate': dense_init(rng_keys[9], D_MODEL, FF_DIM),
        'w_up': dense_init(rng_keys[10], D_MODEL, FF_DIM),
        'w_down': dense_init(rng_keys[11], FF_DIM, D_MODEL),
        'g_in': gain_init(rng_keys[12], D_MODEL),
        'g_q': gain_init(rng_keys[13], HEAD_DIM),
        'g_k': gain_init(rng_keys[14], HEAD_DIM),
        'g_post': gain_init(rng_keys[15], D_MODEL),
        'g_final': gain_init(rng_keys[16], D_MODEL),
    }


def as_bf16(values):
    return values.astype(jnp.bfloat16).astype(jnp.float32)


def norm_rows(values, gain_vec):
    return values * lax.rsqrt(jnp.mean(values * values, axis=-1, keepdims=True) + NORM_EPS) * gain_vec


def rotate(values, angles):
    half_dim = values.shape[-1] // 2
    first_half = values[..., :half_dim]
    second_half = values[..., half_dim:]
    cos_a = jnp.cos(angles)
    sin_a = jnp.sin(angles)
    return jnp.concatenate([first_half * cos_a - second_half * sin_a, second_half * cos_a + first_half * sin_a], axis=-1)


def attend(q_raw, k_raw, v_raw, g_q, g_k, lens):
    n_seq, seq_len, kv_width = k_raw.shape
    n_kv = kv_width // HEAD_DIM
    group_size = q_raw.shape[1] // kv_width
    inv_freq = ROPE_THETA ** (-jnp.arange(0, HEAD_DIM, 2).astype(jnp.float32) / HEAD_DIM)
    key_angle = jnp.arange(seq_len).astype(jnp.float32)[:, None] * inv_freq
    key_rot = norm_rows(k_raw.reshape(n_seq, seq_len, n_kv, HEAD_DIM), g_k)
    key_rot = as_bf16(rotate(key_rot, key_angle[None, :, None, :]))
    q_angle = (lens - 1).astype(jnp.float32)[:, None] * inv_freq
    query_rot = norm_rows(q_raw.reshape(n_seq, n_kv, group_size, HEAD_DIM), g_q)
    query_rot = as_bf16(rotate(query_rot, q_angle[:, None, None, :]))
    scores = jnp.einsum('nkgd,nskd->nkgs', query_rot, key_rot) * HEAD_DIM ** -0.5
    key_valid = jnp.arange(seq_len)[None, :] < lens[:, None]
    scores = jnp.where(key_valid[:, None, None, :], scores, -1e30)
    attn_prob = as_bf16(jax.nn.softmax(scores, axis=-1))
    val_heads = v_raw.reshape(n_seq, seq_len, n_kv, HEAD_DIM)
    attn_mix = jnp.einsum('nkgs,nskd->nkgd', attn_prob, val_heads)
    return as_bf16(attn_mix).reshape(n_seq, q_raw.shape[1])


def embed(hidden, lens, weights):
    w_q, w_k, w_v, w_o, w_gate, w_up, w_down, g_in, g_q, g_k, g_post, g_final = weights
    n_seq, seq_len, model_width = hidden.shape
    x_norm = as_bf16(norm_rows(hidden, g_in))
    x_flat = x_norm.reshape(n_seq * seq_len, model_width)
    k_raw = as_bf16(jnp.dot(x_flat, w_k)).reshape(n_seq, seq_len, -1)
    v_raw = as_bf16(jnp.dot(x_flat, w_v)).reshape(n_seq, seq_len, -1)
    last_idx = (lens - 1)[:, None, None]
    x_last = jnp.take_along_axis(x_norm, last_idx, axis=1)[:, 0]
    h_last = jnp.take_along_axis(hidden, last_idx, axis=1)[:, 0]
    q_raw = as_bf16(jnp.dot(x_last, w_q))
    h_mid = h_last + jnp.dot(attend(q_raw, k_raw, v_raw, g_q, g_k, lens), w_o)
    y_norm = as_bf16(norm_rows(h_mid, g_post))
    gate_val = as_bf16(jnp.dot(y_norm, w_gate))
    up_val = as_bf16(jnp.dot(y_norm, w_up))
    hidden_act = as_bf16(jax.nn.silu(gate_val) * up_val)
    h_out = h_mid + jnp.dot(hidden_act, w_down)
    z_norm = norm_rows(h_out, g_final)
    return z_norm * lax.rsqrt(jnp.sum(z_norm * z_norm, axis=-1, keepdims=True))


def contrast_rows(hid_q, hid_d, len_q, len_d, pos_doc, weights):
    emb_q = embed(hid_q, len_q, weights)
    emb_d = embed(hid_d, len_d, weights)
    logits = jnp.dot(emb_q, emb_d.T) / TEMPERATURE
    log_norm = jax.nn.logsumexp(logits, axis=1)
    pos_logit = jnp.take_along_axis(logits, pos_doc[:, None], axis=1)[:, 0]
    return log_norm - pos_logit


def reference(hid_q, hid_d, len_q, len_d, pos_doc, w_q, w_k, w_v, w_o, w_gate, w_up, w_down, g_in, g_q, g_k, g_post, g_final):
    weights = tuple(weight_in.astype(jnp.float32) for weight_in in (w_q, w_k, w_v, w_o, w_gate, w_up, w_down, g_in, g_q, g_k, g_post, g_final))

    def loss_of(q_float, d_float, weights_f):
        row_losses = contrast_rows(q_float, d_float, len_q, len_d, pos_doc, weights_f)
        return jnp.mean(row_losses), row_losses

    mean_loss, pull_back, loss_rows = jax.vjp(loss_of, hid_q.astype(jnp.float32), hid_d.astype(jnp.float32), weights, has_aux=True)
    d_hid_q, d_hid_d, d_w = pull_back(jnp.ones_like(mean_loss))
    return (loss_rows, d_hid_q.astype(jnp.bfloat16), d_hid_d.astype(jnp.bfloat16), d_w[0], d_w[1], d_w[2], d_w[3], d_w[4], d_w[5], d_w[6], d_w[7], d_w[8], d_w[9], d_w[10], d_w[11])
```

```python
import functools
import jax
import jax.numpy as jnp
from jax import lax
from jax.experimental import pallas as pl
from jax.experimental.pallas import tpu as pltpu
from jax.sharding import PartitionSpec as P

NORM_EPS = 1e-6
ROPE_THETA = 1000000.0
TEMPERATURE = 0.05
HEAD = 128
MAX_QUERY_LEN = 128
F32 = jnp.float32
BF16 = jnp.bfloat16
NT = (((1,), (1,)), ((), ()))
TN = (((0,), (0,)), ((), ()))
NN = (((1,), (0,)), ((), ()))


def mm(lhs, rhs, dims):
    return lax.dot_general(lhs, rhs, dims, preferred_element_type=F32)


def norm_rows(values, gain_vec):
    return values * lax.rsqrt(jnp.mean(values * values, axis=-1, keepdims=True) + NORM_EPS) * gain_vec


def norm_back(values, gain_vec, d_out):
    scale = lax.rsqrt(jnp.mean(values * values, axis=-1, keepdims=True) + NORM_EPS)
    g_dout = d_out * gain_vec
    d_values = scale * g_dout - values * scale ** 3 * jnp.mean(values * g_dout, axis=-1, keepdims=True)
    d_gain = jnp.sum((d_out * values * scale).reshape(-1, values.shape[-1]), axis=0)
    return d_values, d_gain


def rotate(values, angles):
    half_dim = values.shape[-1] // 2
    first_half = values[..., :half_dim]
    second_half = values[..., half_dim:]
    cos_a = jnp.cos(angles)
    sin_a = jnp.sin(angles)
    return jnp.concatenate([first_half * cos_a - second_half * sin_a, second_half * cos_a + first_half * sin_a], axis=-1)


def final_head(h_out, g_final):
    z_norm = norm_rows(h_out, g_final)
    return z_norm * lax.rsqrt(jnp.sum(z_norm * z_norm, axis=-1, keepdims=True))


def swiglu(gate_in, up_in):
    return jax.nn.silu(gate_in) * up_in


def block_queries(q_heads, n_kv):
    n_heads = q_heads.shape[0]
    wide = jnp.concatenate([q_heads] * n_kv, axis=1)
    row = lax.broadcasted_iota(jnp.int32, wide.shape, 0)
    col = lax.broadcasted_iota(jnp.int32, wide.shape, 1)
    return jnp.where(col // HEAD == row // (n_heads // n_kv), wide, 0.0).astype(BF16)


def norm_chunk(h_ref, gin_ref, x_scr, r_scr, start, chunk):
    sub = 32
    for blk in range(chunk // sub):
        rows = pl.ds(pl.multiple_of(start + blk * sub, sub), sub)
        h = h_ref[0, rows, :].astype(F32)
        scale = lax.rsqrt(jnp.mean(h * h, axis=-1, keepdims=True) + NORM_EPS)
        x_scr[rows, :] = (h * scale * gin_ref[...]).astype(BF16)
        if r_scr is not None:
            r_scr[rows, :] = scale


def rotate_keys(k_b, gk, cos, sin):
    k_f = k_b.astype(F32)
    scale = lax.rsqrt(jnp.sum(k_f * k_f, axis=0, keepdims=True) * (1.0 / HEAD) + NORM_EPS)
    k_n = k_f * scale * gk
    half = HEAD // 2
    k1, k2 = k_n[:half], k_n[half:]
    rot = jnp.concatenate([k1 * cos - k2 * sin, k2 * cos + k1 * sin], axis=0)
    return rot.astype(BF16), scale


def fwd_kernel(len_ref, h_ref, wk_ref, q_ref, gin_ref, gk_ref, cos_ref, sin_ref, u_ref, x_scr, kr_scr, s_scr, *, chunk, n_chunk, n_kv):
    length = len_ref[pl.program_id(0)]
    n_heads = q_ref.shape[1]
    q_wide = block_queries(q_ref[0], n_kv)
    s_scr[...] = jnp.full(s_scr.shape, -1e30, F32)
    n_live = (length + chunk - 1) // chunk

    def score(c, carry):
        start = pl.multiple_of(c * chunk, chunk)
        norm_chunk(h_ref, gin_ref, x_scr, None, start, chunk)
        x = x_scr[pl.ds(start, chunk), :]
        for pair in range(n_kv // 2):
            k_pair = mm(wk_ref[pair * 2 * HEAD:(pair + 1) * 2 * HEAD, :], x, NT).astype(BF16)
            for j in range(2):
                for lane in range(chunk // 128):
                    lanes = slice(lane * 128, (lane + 1) * 128)
                    rot, _ = rotate_keys(k_pair[j * HEAD:(j + 1) * HEAD, lanes], gk_ref[...], cos_ref[c, :, lanes], sin_ref[c, :, lanes])
                    base = (pair * 2 + j) * HEAD
                    kr_scr[base:base + HEAD, lanes] = rot
        scores = mm(q_wide, kr_scr[...], NN) * HEAD ** -0.5
        at = start + lax.broadcasted_iota(jnp.int32, scores.shape, 1)
        s_scr[c] = jnp.where(at < length, scores, -1e30)
        return carry

    lax.fori_loop(0, n_live, score, 0)
    s_all = s_scr[...]
    top = jnp.max(jnp.max(s_all, axis=0), axis=-1, keepdims=True)
    p_all = jnp.exp(s_all - top[None])
    total = jnp.sum(jnp.sum(p_all, axis=0), axis=-1, keepdims=True)
    s_scr[...] = p_all / total[None]
    u_ref[0] = jnp.zeros((n_heads, u_ref.shape[2]), F32)

    def mix(c, carry):
        start = pl.multiple_of(c * chunk, chunk)
        u_ref[0] += mm(s_scr[c].astype(BF16), x_scr[pl.ds(start, chunk), :], NN)
        return carry

    lax.fori_loop(0, n_live, mix, 0)


def bwd_kernel(len_ref, tp_ref, h_ref, wk_ref, q_ref, gv_ref, gin_ref, gk_ref, cos_ref, sin_ref,
               dh_ref, dw_ref, dgk_ref, dgin_ref, dq_ref, dxl_ref,
               w_scr, x_scr, r_scr, k_scr, kr_scr, rk_scr, s_scr, dp_scr, dk_scr, dx_scr, *, chunk, n_chunk, n_kv):
    length = len_ref[pl.program_id(0)]
    n_heads = q_ref.shape[1]
    kv_width = n_kv * HEAD
    half_kv = kv_width // 2
    half = HEAD // 2
    q_wide = block_queries(q_ref[0], n_kv)
    n_live = (length + chunk - 1) // chunk

    @pl.when(pl.program_id(0) == 0)
    def _():
        w_scr[:kv_width, :] = wk_ref[...].astype(BF16)
        dw_ref[...] = jnp.zeros(dw_ref.shape, F32)
        dgk_ref[...] = jnp.zeros(dgk_ref.shape, F32)
        dgin_ref[...] = jnp.zeros(dgin_ref.shape, F32)

    w_scr[kv_width:, :] = gv_ref[0].astype(BF16)
    s_scr[...] = jnp.full(s_scr.shape, -1e30, F32)
    dp_scr[...] = jnp.zeros(dp_scr.shape, F32)

    def score(c, carry):
        start = pl.multiple_of(c * chunk, chunk)
        norm_chunk(h_ref, gin_ref, x_scr, r_scr, start, chunk)
        x = x_scr[pl.ds(start, chunk), :]
        for pair in range(n_kv // 2):
            low = pair * 2 * HEAD
            high = low + 2 * HEAD if pair < n_kv // 2 - 1 else kv_width + n_heads
            prod = mm(w_scr[low:high, :], x, NT)
            if pair == n_kv // 2 - 1:
                dp_scr[c] = prod[2 * HEAD:]
            k_pair = prod[:2 * HEAD].astype(BF16)
            k_scr[c, low:low + 2 * HEAD, :] = k_pair
            for j in range(2):
                for lane in range(chunk // 128):
                    lanes = slice(lane * 128, (lane + 1) * 128)
                    rot, scale = rotate_keys(k_pair[j * HEAD:(j + 1) * HEAD, lanes], gk_ref[...], cos_ref[c, :, lanes], sin_ref[c, :, lanes])
                    head = pair * 2 + j
                    kr_scr[c, head * HEAD:(head + 1) * HEAD, lanes] = rot
                    rk_scr[c, head:head + 1, lanes] = scale
        scores = mm(q_wide, kr_scr[c], NN) * HEAD ** -0.5
        at = start + lax.broadcasted_iota(jnp.int32, scores.shape, 1)
        s_scr[c] = jnp.where(at < length, scores, -1e30)
        return carry

    lax.fori_loop(0, n_live, score, 0)
    s_all = s_scr[...]
    top = jnp.max(jnp.max(s_all, axis=0), axis=-1, keepdims=True)
    p_all = jnp.exp(s_all - top[None])
    total = jnp.sum(jnp.sum(p_all, axis=0), axis=-1, keepdims=True)
    p_all = p_all / total[None]
    dp_all = dp_scr[...]
    mean_dp = jnp.sum(jnp.sum(p_all * dp_all, axis=0), axis=-1, keepdims=True)
    s_scr[...] = p_all
    dp_scr[...] = p_all * (dp_all - mean_dp[None]) * HEAD ** -0.5
    dq_ref[0] = jnp.zeros(dq_ref.shape[1:], F32)

    def back(c, carry):
        start = pl.multiple_of(c * chunk, chunk)
        ds_b = dp_scr[c].astype(BF16)
        dk_scr[kv_width:, :] = s_scr[c].astype(BF16)
        dq_ref[0] += mm(ds_b, kr_scr[c], NT)
        gk = gk_ref[...]
        for head in range(n_kv):
            d_rot = mm(q_wide[:, head * HEAD:(head + 1) * HEAD], ds_b, TN)
            for lane in range(chunk // 128):
                lanes = slice(lane * 128, (lane + 1) * 128)
                cos, sin = cos_ref[c, :, lanes], sin_ref[c, :, lanes]
                d1, d2 = d_rot[:half, lanes], d_rot[half:, lanes]
                d_n = jnp.concatenate([d1 * cos + d2 * sin, d2 * cos - d1 * sin], axis=0)
                k_f = k_scr[c, head * HEAD:(head + 1) * HEAD, lanes].astype(F32)
                scale = rk_scr[c, head:head + 1, lanes]
                prod = k_f * d_n
                dgk_ref[...] += prod * scale
                inner = jnp.sum(prod * gk, axis=0, keepdims=True) * (1.0 / HEAD)
                d_k = d_n * gk * scale - k_f * (scale * scale * scale * inner)
                dk_scr[head * HEAD:(head + 1) * HEAD, lanes] = d_k.astype(BF16)
        x = x_scr[pl.ds(start, chunk), :]
        own = pl.multiple_of(tp_ref[0] * half_kv, half_kv)
        dw_ref[...] += mm(dk_scr[pl.ds(own, half_kv), :], x, NN)
        dx_scr[...] = mm(dk_scr[...], w_scr[...], TN)
        sub = 32
        gin = gin_ref[...]
        for blk in range(chunk // sub):
            here = slice(blk * sub, (blk + 1) * sub)
            rows = pl.ds(pl.multiple_of(start + blk * sub, sub), sub)
            h = h_ref[0, rows, :].astype(F32)
            scale = r_scr[rows, :]
            d_x = dx_scr[here, :]
            g_dx = d_x * gin
            inner = jnp.mean(h * g_dx, axis=-1, keepdims=True)
            dh_ref[0, rows, :] = (scale * g_dx - h * (scale * scale * scale * inner)).astype(BF16)
            dgin_ref[...] += jnp.sum((d_x * h * scale).reshape(sub // 8, 8, h.shape[1]), axis=0)

        @pl.when((length - 1) // chunk == c)
        def _():
            dxl_ref[0] = dx_scr[pl.ds(length - 1 - start, 1), :]

        return carry

    lax.fori_loop(0, n_live, back, 0)
    for c in range(1, n_chunk):
        @pl.when(c >= n_live)
        def _():
            dh_ref[0, c * chunk:(c + 1) * chunk, :] = jnp.zeros((chunk, dh_ref.shape[2]), BF16)
    tail = dh_ref.shape[1] - n_chunk * chunk
    if tail:
        dh_ref[0, n_chunk * chunk:, :] = jnp.zeros((tail, dh_ref.shape[2]), BF16)


def outer_kernel(a_ref, b_ref, o_ref):
    o_ref[...] = mm(a_ref[...].astype(BF16), b_ref[...].astype(BF16), TN)


def outer_sum(rows_a, at_a, rows_b, n_cols):
    n_rows, width = rows_b.shape
    block = min(256, width)
    return pl.pallas_call(
        outer_kernel,
        grid=(width // block,),
        in_specs=[pl.BlockSpec((n_rows, n_cols), lambda i: (0, at_a)), pl.BlockSpec((n_rows, block), lambda i: (0, i))],
        out_specs=pl.BlockSpec((n_cols, block), lambda i: (0, i)),
        out_shape=jax.ShapeDtypeStruct((n_cols, width), F32),
        cost_estimate=pl.CostEstimate(flops=2 * n_rows * n_cols * width, bytes_accessed=4 * n_rows * (n_cols + width), transcendentals=0),
        name="outer_sum",
    )(rows_a, rows_b)


def value_kernel(d_ref, w_ref, o_ref):
    o_ref[...] = mm(d_ref[...].astype(BF16), w_ref[0].astype(BF16), NN)


def value_rows(d_heads, wv_heads, group):
    n_seq, total = d_heads.shape
    n_heads, width = total // HEAD, wv_heads.shape[2]
    out = pl.pallas_call(
        value_kernel,
        grid=(n_heads,),
        in_specs=[pl.BlockSpec((n_seq, HEAD), lambda i: (0, i)), pl.BlockSpec((1, HEAD, width), lambda i: (i // group, 0, 0))],
        out_specs=pl.BlockSpec((n_seq, width), lambda i: (0, i)),
        out_shape=jax.ShapeDtypeStruct((n_seq, n_heads * width), F32),
        cost_estimate=pl.CostEstimate(flops=2 * n_seq * total * width, bytes_accessed=4 * n_seq * n_heads * width, transcendentals=0),
        name="value_rows",
    )(d_heads, wv_heads)
    return out.reshape(n_seq, n_heads, width)


def rope_tables(n_chunk, chunk):
    inv_freq = ROPE_THETA ** (-jnp.arange(0, HEAD, 2, dtype=F32) / HEAD)
    angle = inv_freq[:, None] * jnp.arange(n_chunk * chunk, dtype=F32)[None, :]
    split = lambda t: t.reshape(HEAD // 2, n_chunk, chunk).transpose(1, 0, 2)
    return split(jnp.cos(angle)), split(jnp.sin(angle))


def whole(shape):
    return pl.BlockSpec(shape, lambda *_: (0,) * len(shape))


def per_seq(shape):
    return pl.BlockSpec((1,) + shape, lambda i, *_: (i,) + (0,) * len(shape))


def run_forward(hidden, lens, wk_t, q_heads, g_in, g_k, span, chunk):
    n_seq, _, width = hidden.shape
    n_heads = q_heads.shape[1]
    kv_width = wk_t.shape[0]
    n_chunk = span // chunk
    cos, sin = rope_tables(n_chunk, chunk)
    gk = jnp.broadcast_to(g_k[:, None], (HEAD, 128))
    tokens = n_seq * span
    return pl.pallas_call(
        functools.partial(fwd_kernel, chunk=chunk, n_chunk=n_chunk, n_kv=kv_width // HEAD),
        grid_spec=pltpu.PrefetchScalarGridSpec(
            num_scalar_prefetch=1,
            grid=(n_seq,),
            in_specs=[per_seq((span, width)), whole(wk_t.shape), per_seq((n_heads, HEAD)), whole((1, width)), whole(gk.shape), whole(cos.shape), whole(sin.shape)],
            out_specs=per_seq((n_heads, width)),
            scratch_shapes=[pltpu.VMEM((span, width), BF16), pltpu.VMEM((kv_width, chunk), BF16), pltpu.VMEM((n_chunk, n_heads, chunk), F32)],
        ),
        out_shape=jax.ShapeDtypeStruct((n_seq, n_heads, width), F32),
        compiler_params=pltpu.CompilerParams(dimension_semantics=("arbitrary",), vmem_limit_bytes=56 * 1024 * 1024),
        cost_estimate=pl.CostEstimate(flops=2 * tokens * width * kv_width, bytes_accessed=2 * tokens * width, transcendentals=0),
        name="attend_forward",
    )(lens, hidden, wk_t, q_heads, g_in[None, :], gk, cos, sin)


def run_backward(hidden, lens, tp_index, wk_all, q_heads, g_val, g_in, g_k, span, chunk):
    n_seq, seq_len, width = hidden.shape
    n_heads = q_heads.shape[1]
    kv_width = wk_all.shape[0]
    n_kv = kv_width // HEAD
    n_chunk = span // chunk
    cos, sin = rope_tables(n_chunk, chunk)
    gk = jnp.broadcast_to(g_k[:, None], (HEAD, 128))
    tokens = n_seq * span
    sds = jax.ShapeDtypeStruct
    return pl.pallas_call(
        functools.partial(bwd_kernel, chunk=chunk, n_chunk=n_chunk, n_kv=n_kv),
        grid_spec=pltpu.PrefetchScalarGridSpec(
            num_scalar_prefetch=2,
            grid=(n_seq,),
            in_specs=[per_seq((span, width)), whole(wk_all.shape), per_seq((n_heads, HEAD)), per_seq((n_heads, width)), whole((1, width)), whole(gk.shape), whole(cos.shape), whole(sin.shape)],
            out_specs=[per_seq((seq_len, width)), whole((kv_width // 2, width)), whole((HEAD, 128)), whole((8, width)), per_seq((n_heads, kv_width)), per_seq((1, width))],
            scratch_shapes=[
                pltpu.VMEM((kv_width + n_heads, width), BF16),
                pltpu.VMEM((span, width), BF16),
                pltpu.VMEM((span, 1), F32),
                pltpu.VMEM((n_chunk, kv_width, chunk), BF16),
                pltpu.VMEM((n_chunk, kv_width, chunk), BF16),
                pltpu.VMEM((n_chunk, n_kv, chunk), F32),
                pltpu.VMEM((n_chunk, n_heads, chunk), F32),
                pltpu.VMEM((n_chunk, n_heads, chunk), F32),
                pltpu.VMEM((kv_width + n_heads, chunk), BF16),
                pltpu.VMEM((chunk, width), F32),
            ],
        ),
        out_shape=[sds((n_seq, seq_len, width), BF16), sds((kv_width // 2, width), F32), sds((HEAD, 128), F32), sds((8, width), F32), sds((n_seq, n_heads, kv_width), F32), sds((n_seq, 1, width), F32)],
        compiler_params=pltpu.CompilerParams(dimension_semantics=("arbitrary",), vmem_limit_bytes=56 * 1024 * 1024),
        cost_estimate=pl.CostEstimate(flops=5 * tokens * width * kv_width, bytes_accessed=4 * tokens * width, transcendentals=0),
        name="attend_backward",
    )(lens, tp_index, hidden, wk_all, q_heads, g_val, g_in[None, :], gk, cos, sin)


def patch_kernel(len_ref, rows_ref, src_ref, dst_ref, tiles, sem_in, sem_out, *, n_seq, tile):
    def place(i):
        at = pl.multiple_of(((len_ref[i] - 1) // tile) * tile, tile)
        return src_ref.at[i, pl.ds(at, tile), :], dst_ref.at[i, pl.ds(at, tile), :]

    def fetch(i, carry):
        pltpu.make_async_copy(place(i)[0], tiles.at[i], sem_in.at[i]).start()
        return carry

    def change(i, carry):
        source, target = place(i)
        pltpu.make_async_copy(source, tiles.at[i], sem_in.at[i]).wait()
        row = lax.broadcasted_iota(jnp.int32, tiles.shape[1:], 0)
        new = jnp.broadcast_to(rows_ref[i], tiles.shape[1:])
        tiles[i] = jnp.where(row == (len_ref[i] - 1) % tile, new, tiles[i].astype(F32)).astype(BF16)
        pltpu.make_async_copy(tiles.at[i], target, sem_out.at[i]).start()
        return carry

    def drain(i, carry):
        pltpu.make_async_copy(tiles.at[i], place(i)[1], sem_out.at[i]).wait()
        return carry

    lax.fori_loop(0, n_seq, fetch, 0)
    lax.fori_loop(0, n_seq, change, 0)
    lax.fori_loop(0, n_seq, drain, 0)


def patch_rows(d_hidden, lens, rows):
    n_seq, _, width = d_hidden.shape
    tile = 16
    return pl.pallas_call(
        functools.partial(patch_kernel, n_seq=n_seq, tile=tile),
        in_specs=[pl.BlockSpec(memory_space=pltpu.SMEM), pl.BlockSpec(memory_space=pltpu.VMEM), pl.BlockSpec(memory_space=pl.ANY)],
        out_specs=pl.BlockSpec(memory_space=pl.ANY),
        scratch_shapes=[pltpu.VMEM((n_seq, tile, width), BF16), pltpu.SemaphoreType.DMA((n_seq,)), pltpu.SemaphoreType.DMA((n_seq,))],
        out_shape=jax.ShapeDtypeStruct(d_hidden.shape, BF16),
        input_output_aliases={2: 0},
        name="patch_last_rows",
    )(lens, rows[:, None, :], d_hidden)


def solution(mesh):
    dp_size = mesh.shape['dp']
    tp_size = mesh.shape['tp']
    swap = [(i, (i + 1) % tp_size) for i in range(tp_size)]

    def tp_sum(value):
        return value + lax.ppermute(value, 'tp', swap)

    def device_step(hid_q, hid_d, len_q, len_d, pos_doc, w_q, w_k, w_v, w_o, w_gate, w_up, w_down, g_in, g_q, g_k, g_post, g_final):
        g_in, g_q, g_k, g_post, g_final = (g.astype(F32) for g in (g_in, g_q, g_k, g_post, g_final))
        n_q, n_d = hid_q.shape[0], hid_d.shape[0]
        n_own = n_q + n_d
        width = hid_q.shape[2]
        n_kv = w_k.shape[1] // HEAD
        n_heads = w_q.shape[1] // HEAD
        group = n_heads // n_kv
        tp_i = lax.axis_index('tp')
        dp_i = lax.axis_index('dp')
        span_q, span_d = min(MAX_QUERY_LEN, hid_q.shape[1]), hid_d.shape[1]
        n_query = n_q * dp_size

        wk_t, wv_t = w_k.T, w_v.T
        kv_all = lax.all_gather(jnp.stack([wk_t, wv_t]).astype(F32)[None], 'tp', axis=0, tiled=True)
        wk_all = kv_all[:, 0].reshape(-1, width)
        wv_all = kv_all[:, 1].reshape(tp_size * n_kv, HEAD, width)

        lens = jnp.concatenate([len_q, len_d])
        h_last = jnp.concatenate([
            jnp.take_along_axis(hid, (ln - 1)[:, None, None], axis=1)[:, 0] for hid, ln in ((hid_q, len_q), (hid_d, len_d))
        ]).astype(F32)
        x_last = lax.reduce_precision(norm_rows(h_last, g_in), 8, 7)
        q_raw = mm(x_last.astype(BF16), w_q, NN).astype(BF16)
        inv_freq = ROPE_THETA ** (-jnp.arange(0, HEAD, 2, dtype=F32) / HEAD)
        q_angle = (lens - 1).astype(F32)[:, None, None] * inv_freq

        def rotate_query(raw, gain):
            return rotate(norm_rows(raw, gain), q_angle)

        q_rot, q_pull = jax.vjp(rotate_query, q_raw.astype(F32).reshape(n_own, n_heads, HEAD), g_q)
        q_rot = lax.reduce_precision(q_rot, 8, 7)
        q_all = lax.all_gather(q_rot, 'tp', axis=1, tiled=True)

        u = jnp.concatenate([
            run_forward(hid_q, len_q, wk_t, q_rot[:n_q], g_in, g_k, span_q, min(128, span_q)),
            run_forward(hid_d, len_d, wk_t, q_rot[n_q:], g_in, g_k, span_d, min(256, span_d)),
        ])
        u_b = u.astype(BF16).reshape(n_own, n_kv, group, width)
        wv_heads = w_v.reshape(width, n_kv, HEAD)
        attn_out = jnp.einsum('nkgd,dke->nkge', u_b, wv_heads, preferred_element_type=F32).reshape(n_own, -1)
        attn_out = lax.reduce_precision(attn_out, 8, 7)
        h_mid = h_last + tp_sum(mm(attn_out.astype(BF16), w_o, NN))

        def gate_up(rows):
            y = norm_rows(rows, g_post).astype(BF16)
            return y, mm(y, w_gate, NN).astype(BF16), mm(y, w_up, NN).astype(BF16)

        _, gate_own, up_own = gate_up(h_mid)
        act_own = swiglu(gate_own.astype(F32), up_own.astype(F32)).astype(BF16)
        h_out = h_mid + tp_sum(mm(act_own, w_down, NN))

        note = jnp.zeros((8, 2 * width), F32).at[0, :n_q].set(pos_doc.astype(F32))
        rows_all = lax.all_gather(jnp.concatenate([jnp.concatenate([h_mid, h_out], axis=1), note]), 'dp', axis=0, tiled=False)
        side_all = lax.all_gather(jnp.concatenate([x_last, attn_out], axis=1), 'dp', axis=0, tiled=True)
        pos_all = rows_all[:, n_own, :n_q].reshape(-1).astype(jnp.int32)
        seq_rows = jnp.concatenate([rows_all[:, :n_q].reshape(-1, 2 * width), rows_all[:, n_q:n_own].reshape(-1, 2 * width)])
        mid_all, out_all = seq_rows[:, :width], seq_rows[:, width:]

        emb_all, head_pull = jax.vjp(final_head, out_all, g_final)
        emb_q, emb_d = emb_all[:n_query], emb_all[n_query:]
        logits = jnp.einsum('qd,kd->qk', emb_q, emb_d, precision=lax.Precision.HIGHEST) / TEMPERATURE
        log_norm = jax.nn.logsumexp(logits, axis=1)
        is_pos = jnp.arange(emb_d.shape[0])[None, :] == pos_all[:, None]
        loss_all = log_norm - jnp.sum(jnp.where(is_pos, logits, 0.0), axis=1)
        loss_rows = lax.dynamic_slice_in_dim(loss_all, dp_i * n_q, n_q)
        d_logits = (jnp.exp(logits - log_norm[:, None]) - is_pos.astype(F32)) / (n_query * TEMPERATURE)
        d_emb_q = jnp.einsum('qk,kd->qd', d_logits, emb_d, precision=lax.Precision.HIGHEST)
        d_emb_d = jnp.einsum('qk,qd->kd', d_logits, emb_q, precision=lax.Precision.HIGHEST)
        d_out_all, d_gfinal = head_pull(jnp.concatenate([d_emb_q, d_emb_d]))

        def own_rows(all_rows):
            return jnp.concatenate([
                lax.dynamic_slice_in_dim(all_rows, dp_i * n_q, n_q),
                lax.dynamic_slice_in_dim(all_rows, n_query + dp_i * n_d, n_d),
            ])

        y_all, gate_all, up_all = gate_up(mid_all)
        act_all, act_pull = jax.vjp(swiglu, gate_all.astype(F32), up_all.astype(F32))
        d_out_b = d_out_all.astype(BF16)
        d_act = mm(d_out_b, w_down, NT).astype(BF16)
        d_gate, d_up = (d.astype(BF16) for d in act_pull(d_act.astype(F32)))
        d_wdown = mm(act_all.astype(BF16), d_out_b, TN)
        d_wgate = mm(y_all, d_gate, TN)
        d_wup = mm(y_all, d_up, TN)
        d_y = tp_sum(mm(own_rows(d_gate), w_gate, NT) + mm(own_rows(d_up), w_up, NT))
        d_ymid, d_gpost = norm_back(h_mid, g_post, d_y)
        d_hmid = own_rows(d_out_all) + d_ymid

        d_attn = lax.reduce_precision(mm(d_hmid.astype(BF16), w_o, NT), 8, 7)
        d_attn_all = lax.all_gather(d_attn, 'tp', axis=1, tiled=True)
        g_val = value_rows(d_attn_all, wv_all, group)
        d_wv = jnp.einsum('nkgd,nkge->dke', u_b, d_attn.astype(BF16).reshape(n_own, n_kv, group, HEAD), preferred_element_type=F32).reshape(width, -1)
        d_wv = lax.psum(d_wv, 'dp')
        d_hmid_all = lax.all_gather(d_hmid, 'dp', axis=0, tiled=True)
        d_wo = outer_sum(side_all, 1, d_hmid_all, width)

        tp_arr = tp_i.astype(jnp.int32)[None]
        back_q = run_backward(hid_q, len_q, tp_arr, wk_all, q_all[:n_q], g_val[:n_q], g_in, g_k, span_q, min(128, span_q))
        back_d = run_backward(hid_d, len_d, tp_arr, wk_all, q_all[n_q:], g_val[n_q:], g_in, g_k, span_d, min(256, span_d))
        d_wk_t = back_q[1] + back_d[1]
        d_gk = jnp.sum(back_q[2] + back_d[2], axis=1)
        d_gin = jnp.sum(back_q[3] + back_d[3], axis=0)
        d_rot = jnp.concatenate([back_q[4], back_d[4]]).reshape(n_own, tp_size * n_kv, group, tp_size * n_kv, HEAD)
        d_rot = jnp.sum(jnp.where(jnp.eye(tp_size * n_kv, dtype=bool)[None, :, None, :, None], d_rot, 0.0), axis=3)
        d_rot = lax.dynamic_slice_in_dim(d_rot.reshape(n_own, -1, HEAD), tp_i * n_heads, n_heads, axis=1)
        d_x_row = jnp.concatenate([back_q[5], back_d[5]])[:, 0]

        d_qraw, d_gq = q_pull(d_rot)
        d_qraw = lax.reduce_precision(d_qraw.reshape(n_own, -1), 8, 7)
        gq_row = jnp.zeros((8, width), F32).at[0, :HEAD].set(d_gq)
        both = tp_sum(jnp.concatenate([mm(d_qraw.astype(BF16), w_q, NT), gq_row]))
        d_xlast, d_gq = both[:n_own], both[n_own, :HEAD]
        row_back, _ = norm_back(h_last, g_in, d_x_row + d_xlast)
        d_gin = d_gin + jnp.sum(d_xlast * norm_rows(h_last, 1.0), axis=0)
        last_rows = row_back + d_hmid
        d_hid_q = patch_rows(back_q[0], len_q, last_rows[:n_q])
        d_hid_d = patch_rows(back_d[0], len_d, last_rows[n_q:])

        d_qraw_all = lax.all_gather(d_qraw, 'dp', axis=0, tiled=True)
        d_wq = outer_sum(side_all, 0, d_qraw_all, width)
        gains = jnp.stack([d_gin, d_gpost, jnp.pad(jnp.concatenate([d_gq, d_gk]), (0, width - 2 * HEAD))])
        summed = lax.psum(jnp.concatenate([d_wk_t, jnp.pad(gains, ((0, 5), (0, 0)))]), 'dp')
        n_rows = d_wk_t.shape[0]
        d_wk = summed[:n_rows].T
        d_gin, d_gpost, heads = summed[n_rows], summed[n_rows + 1], summed[n_rows + 2]
        return (loss_rows, d_hid_q, d_hid_d, d_wq, d_wk, d_wv, d_wo, d_wgate, d_wup, d_wdown, d_gin, heads[:HEAD], heads[HEAD:2 * HEAD], d_gpost, d_gfinal)

    col_split = P(None, 'tp')
    row_split = P('tp', None)
    in_specs = (P('dp'), P('dp'), P('dp'), P('dp'), P('dp'), col_split, col_split, col_split, row_split, col_split, col_split, row_split, P(), P(), P(), P(), P())
    out_specs = (P('dp'), P('dp'), P('dp'), col_split, col_split, col_split, row_split, col_split, col_split, row_split, P(), P(), P(), P(), P())
    return jax.shard_map(device_step, mesh=mesh, in_specs=in_specs, out_specs=out_specs, check_vma=False)
```
